32 devices in a mesh: inst: 2 (over x), dev: 4 (over z), side: 4 (over y, core).
Axes of the slice: x: 2, y: 2, z: 4, core: 2. Of those that a mesh axis runs over, the one named last changes fastest.
Arguments:
- hidden: bfloat16 [256, 2048], P(('inst', 'dev')), parts along dimension 0
- k_cache: bfloat16 [1, 256, 16, 128, 128], P(None, ('inst', 'dev')), parts along dimension 1
- v_cache: bfloat16 [1, 256, 16, 128, 128], P(None, ('inst', 'dev')), parts along dimension 1
- cache_lens: int32 [256], P(('inst', 'dev')), parts along dimension 0
- expert_ids: int32 [1, 256, 4], P(None, ('inst', 'dev')), parts along dimension 1
- route_gates: float32 [1, 256, 4], P(None, ('inst', 'dev')), parts along dimension 1
- attn_gain: float32 [1, 2048], replicated
- ffn_gain: float32 [1, 2048], replicated
- w_q: bfloat16 [1, 2048, 2048], replicated
- w_kv: bfloat16 [1, 2048, 4096], replicated
- w_o: bfloat16 [1, 2048, 2048], replicated
- shared_gate: bfloat16 [1, 2048, 5632], replicated
- shared_up: bfloat16 [1, 2048, 5632], replicated
- shared_down: bfloat16 [1, 5632, 2048], replicated
- w_gate: bfloat16 [1, 60, 2048, 1408], P(None, 'dev')
- w_up: bfloat16 [1, 60, 2048, 1408], P(None, 'dev')
- w_down: bfloat16 [1, 60, 1408, 2048], P(None, 'dev')
Outputs:
- output: bfloat16 [256, 2048], P(('inst', 'dev')), parts along dimension 0
There are 2 independent parts. The reference program is written for one: setup_inputs(seed, part) draws one part's arguments, and reference() takes and returns one part's arrays. A program takes and returns all parts, laid end to end along the dimension named above; an argument that names none is the same for every part.
All inputs are finite; a program needn't handle non-finite values.
Results may differ from the reference program's by a relative error of at most 0.0154421.
Values are sent between devices in bfloat16 or wider.
A program may use at most 1.5 GiB of HBM per device.

```python
import jax
import jax.numpy as jnp
import math
from jax import lax

MODEL_DIM = 2048
Q_HEADS = 16
KV_HEADS = 16
HEAD_DIM = 128
NUM_EXPERTS = 60
EXPERT_FF = 1408
TOP_K = 4
SHARED_FF = 5632
NUM_LAYERS = 1
CACHE_LEN = 128
BLOCK_TOKENS = 16
NUM_BLOCKS = 8

BATCH = BLOCK_TOKENS * NUM_BLOCKS
EXPERT_CAP = 2 * (BLOCK_TOKENS * TOP_K // NUM_EXPERTS) - 1 + min(1, BLOCK_TOKENS * TOP_K % NUM_EXPERTS)
TOTAL_CAP = NUM_BLOCKS * EXPERT_CAP
NORM_EPS = 1e-6
ROPE_BASE = 10000.0


def draw_routes(route_key):
    total = BLOCK_TOKENS * TOP_K
    base_count = total // NUM_EXPERTS
    spare = total % NUM_EXPERTS
    key_perm, key_shift, key_tok = jax.random.split(route_key, 3)
    expert_order = jax.random.permutation(key_perm, NUM_EXPERTS)
    shifts = jax.random.randint(key_shift, (NUM_EXPERTS // 2,), 0, base_count)
    shifts = shifts.at[0].set(base_count - 1)
    deltas = jnp.stack([shifts, -shifts], axis=1).reshape(NUM_EXPERTS)
    extras = (jnp.arange(NUM_EXPERTS) < spare).astype(jnp.int32)
    counts = jnp.zeros((NUM_EXPERTS,), jnp.int32).at[expert_order].set(base_count + deltas + extras)
    run_ends = jnp.cumsum(counts)
    places = jnp.arange(total)
    expert_of = jnp.sum((run_ends[None, :] <= places[:, None]).astype(jnp.int32), axis=1)
    by_place = expert_of.reshape(TOP_K, BLOCK_TOKENS).T
    tok_order = jax.random.permutation(key_tok, BLOCK_TOKENS)
    return by_place[tok_order]


def setup_inputs(seed: int = 0, part: int = 0) -> dict:
    root_key = jax.random.key(seed)
    part_keys = jax.random.split(jax.random.fold_in(root_key, part), 7)
    shared_keys = jax.random.split(root_key, 11)
    q_width = Q_HEADS * HEAD_DIM
    kv_width = KV_HEADS * HEAD_DIM
    key_scale = (0.5 * math.log(CACHE_LEN)) ** 0.5
    dim_scale = MODEL_DIM ** -0.5
    cache_shape = (NUM_LAYERS, BATCH, KV_HEADS, CACHE_LEN, HEAD_DIM)
    hidden = jax.random.normal(part_keys[0], (BATCH, MODEL_DIM), jnp.float32).astype(jnp.bfloat16)
    k_cache = (key_scale * jax.random.normal(part_keys[1], cache_shape, jnp.float32)).astype(jnp.bfloat16)
    v_mean = jax.random.normal(part_keys[2], (NUM_LAYERS, BATCH, KV_HEADS, 1, HEAD_DIM), jnp.float32)
    v_cache = (0.6 * v_mean + 0.8 * jax.random.normal(part_keys[3], cache_shape, jnp.float32)).astype(jnp.bfloat16)
    cache_lens = jax.random.randint(part_keys[4], (BATCH,), CACHE_LEN // 4, CACHE_LEN + 1)
    cache_lens = cache_lens.at[0].set(CACHE_LEN).at[1].set(CACHE_LEN // 4)
    route_keys = jax.random.split(part_keys[5], NUM_LAYERS * NUM_BLOCKS)
    expert_ids = jax.vmap(draw_routes)(route_keys).reshape(NUM_LAYERS, BATCH, TOP_K)
    route_gates = jax.random.uniform(part_keys[6], (NUM_LAYERS, BATCH, TOP_K), jnp.float32, 0.3, 1.0)
    attn_gain = jax.random.uniform(shared_keys[0], (NUM_LAYERS, MODEL_DIM), jnp.float32, 0.5, 1.5)
    ffn_gain = jax.random.uniform(shared_keys[1], (NUM_LAYERS, MODEL_DIM), jnp.float32, 0.5, 1.5)
    w_q = (dim_scale * jax.random.normal(shared_keys[2], (NUM_LAYERS, MODEL_DIM, q_width), jnp.float32)).astype(jnp.bfloat16)
    kv_cols = jnp.array([key_scale, CACHE_LEN / 8.0], jnp.float32)[None, None, :, None] * dim_scale
    w_kv = (kv_cols * jax.random.normal(shared_keys[3], (NUM_LAYERS, MODEL_DIM, 2, kv_width), jnp.float32)).reshape(NUM_LAYERS, MODEL_DIM, 2 * kv_width).astype(jnp.bfloat16)
    w_o = (q_width ** -0.5 * jax.random.normal(shared_keys[4], (NUM_LAYERS, q_width, MODEL_DIM), jnp.float32)).astype(jnp.bfloat16)
    shared_gate = (dim_scale * jax.random.normal(shared_keys[5], (NUM_LAYERS, MODEL_DIM, SHARED_FF), jnp.float32)).astype(jnp.bfloat16)
    shared_up = (dim_scale * jax.random.normal(shared_keys[6], (NUM_LAYERS, MODEL_DIM, SHARED_FF), jnp.float32)).astype(jnp.bfloat16)
    shared_down = (SHARED_FF ** -0.5 * jax.random.normal(shared_keys[7], (NUM_LAYERS, SHARED_FF, MODEL_DIM), jnp.float32)).astype(jnp.bfloat16)
    w_gate = (dim_scale * jax.random.normal(shared_keys[8], (NUM_LAYERS, NUM_EXPERTS, MODEL_DIM, EXPERT_FF), jnp.float32)).astype(jnp.bfloat16)
    w_up = (dim_scale * jax.random.normal(shared_keys[9], (NUM_LAYERS, NUM_EXPERTS, MODEL_DIM, EXPERT_FF), jnp.float32)).astype(jnp.bfloat16)
    w_down = (EXPERT_FF ** -0.5 * jax.random.normal(shared_keys[10], (NUM_LAYERS, NUM_EXPERTS, EXPERT_FF, MODEL_DIM), jnp.float32)).astype(jnp.bfloat16)
    return {'hidden': hidden, 'k_cache': k_cache, 'v_cache': v_cache, 'cache_lens': cache_lens, 'expert_ids': expert_ids, 'route_gates': route_gates, 'attn_gain': attn_gain, 'ffn_gain': ffn_gain, 'w_q': w_q, 'w_kv': w_kv, 'w_o': w_o, 'shared_gate': shared_gate, 'shared_up': shared_up, 'shared_down': shared_down, 'w_gate': w_gate, 'w_up': w_up, 'w_down': w_down}


def rms_norm(in_rows, norm_gain):
    rows_f = in_rows.astype(jnp.float32)
    inv_rms = lax.rsqrt(jnp.mean(rows_f * rows_f, axis=-1, keepdims=True) + NORM_EPS)
    return (rows_f * inv_rms * norm_gain).astype(jnp.bfloat16)


def rotate_pos(in_vecs, positions):
    half_dim = in_vecs.shape[-1] // 2
    inv_freq = ROPE_BASE ** (-jnp.arange(half_dim, dtype=jnp.float32) * 2.0 / in_vecs.shape[-1])
    angles = positions.astype(jnp.float32)[:, None] * inv_freq[None, :]
    cosine = jnp.cos(angles)[:, None, :]
    sine_part = jnp.sin(angles)[:, None, :]
    first_half = in_vecs[..., :half_dim]
    second = in_vecs[..., half_dim:]
    return jnp.concatenate([first_half * cosine - second * sine_part, second * cosine + first_half * sine_part], axis=-1)


def swiglu(in_rows, gate_w, up_w, down_w):
    act_gate = jnp.dot(in_rows, gate_w, preferred_element_type=jnp.float32)
    act_up = jnp.dot(in_rows, up_w, preferred_element_type=jnp.float32)
    inner_act = (jax.nn.silu(act_gate) * act_up).astype(jnp.bfloat16)
    return jnp.dot(inner_act, down_w, preferred_element_type=jnp.float32).astype(jnp.bfloat16)


def attend_block(blk_pack, wq_l, wkv_l, wo_l):
    in_rows, key_blk, val_blk, lens_blk = blk_pack
    tokens = in_rows.shape[0]
    groups = Q_HEADS // KV_HEADS
    q_rows = jnp.dot(in_rows, wq_l, preferred_element_type=jnp.float32).astype(jnp.bfloat16)
    fresh_kv = jnp.dot(in_rows, wkv_l, preferred_element_type=jnp.float32).astype(jnp.bfloat16).reshape(tokens, 2, KV_HEADS, HEAD_DIM)
    q_rows = rotate_pos(q_rows.astype(jnp.float32).reshape(tokens, Q_HEADS, HEAD_DIM), lens_blk).astype(jnp.bfloat16).reshape(tokens, KV_HEADS, groups, HEAD_DIM)
    new_key = rotate_pos(fresh_kv[:, 0].astype(jnp.float32), lens_blk).astype(jnp.bfloat16)
    new_val = fresh_kv[:, 1]
    score_scale = HEAD_DIM ** -0.5
    scores = jnp.einsum('tkgd,tksd->tkgs', q_rows.astype(jnp.float32), key_blk.astype(jnp.float32)) * score_scale
    valid_mask = jnp.arange(CACHE_LEN)[None, None, None, :] < lens_blk[:, None, None, None]
    scores = jnp.where(valid_mask, scores, -jnp.inf)
    self_score = jnp.einsum('tkgd,tkd->tkg', q_rows.astype(jnp.float32), new_key.astype(jnp.float32)) * score_scale
    peak_score = jnp.maximum(jnp.max(scores, axis=-1), self_score)
    weights = jnp.exp(scores - peak_score[..., None])
    self_weight = jnp.exp(self_score - peak_score)
    denom_sum = jnp.sum(weights, axis=-1) + self_weight
    prob_bf = (weights / denom_sum[..., None]).astype(jnp.bfloat16)
    self_prob = (self_weight / denom_sum).astype(jnp.bfloat16)
    context = jnp.einsum('tkgs,tksd->tkgd', prob_bf.astype(jnp.float32), val_blk.astype(jnp.float32))
    context = context + self_prob.astype(jnp.float32)[..., None] * new_val.astype(jnp.float32)[:, :, None, :]
    context = context.astype(jnp.bfloat16).reshape(tokens, Q_HEADS * HEAD_DIM)
    return jnp.dot(context, wo_l, preferred_element_type=jnp.float32)


def reference(hidden, k_cache, v_cache, cache_lens, expert_ids, route_gates, attn_gain, ffn_gain, w_q, w_kv, w_o, shared_gate, shared_up, shared_down, w_gate, w_up, w_down):
    lens_blocks = cache_lens.reshape(NUM_BLOCKS, BLOCK_TOKENS)
    expert_range = jnp.arange(NUM_EXPERTS)
    owner_idx = jnp.arange(BATCH * TOP_K) // TOP_K

    def layer_step(x_state, layer_pack):
        keys_l, vals_l, ids_l, gates_l, gain_a, gain_f, wq_l, wkv_l, wo_l, sg_l, su_l, sd_l, eg_l, eu_l, ed_l = layer_pack
        normed = rms_norm(x_state, gain_a)
        block_pack = (normed.reshape(NUM_BLOCKS, BLOCK_TOKENS, MODEL_DIM), keys_l.reshape(NUM_BLOCKS, BLOCK_TOKENS, KV_HEADS, CACHE_LEN, HEAD_DIM), vals_l.reshape(NUM_BLOCKS, BLOCK_TOKENS, KV_HEADS, CACHE_LEN, HEAD_DIM), lens_blocks)
        attn_out = lax.map(lambda blk_pack: attend_block(blk_pack, wq_l, wkv_l, wo_l), block_pack).reshape(BATCH, MODEL_DIM)
        mid_rows = (x_state.astype(jnp.float32) + attn_out).astype(jnp.bfloat16)
        ffn_in = rms_norm(mid_rows, gain_f)
        shared_out = swiglu(ffn_in, sg_l, su_l, sd_l)
        flat_ids = ids_l.reshape(BATCH * TOP_K)
        onehot = (flat_ids[:, None] == expert_range[None, :]).astype(jnp.int32)
        slot_ids = jnp.sum((jnp.cumsum(onehot, axis=0) - onehot) * onehot, axis=1)
        slot_table = jnp.zeros((NUM_EXPERTS, TOTAL_CAP), jnp.int32).at[flat_ids, slot_ids].set(owner_idx)
        expert_rows = ffn_in[slot_table]
        expert_out = lax.map(lambda expert_pack: swiglu(expert_pack[0], expert_pack[1], expert_pack[2], expert_pack[3]), (expert_rows, eg_l, eu_l, ed_l))
        picked = expert_out[flat_ids, slot_ids].reshape(BATCH, TOP_K, MODEL_DIM)
        routed = jnp.sum(gates_l[:, :, None] * picked.astype(jnp.float32), axis=1)
        new_state = (mid_rows.astype(jnp.float32) + shared_out.astype(jnp.float32) + routed).astype(jnp.bfloat16)
        return new_state, None

    layer_stack = (k_cache, v_cache, expert_ids, route_gates, attn_gain, ffn_gain, w_q, w_kv, w_o, shared_gate, shared_up, shared_down, w_gate, w_up, w_down)
    return lax.scan(layer_step, hidden, layer_stack)[0]
```

```python
import functools
import math

import jax
import jax.numpy as jnp
from jax import lax
from jax.experimental import pallas as pl
from jax.experimental.pallas import tpu as pltpu
from jax.sharding import PartitionSpec as P

NORM_EPS = 1e-6
ROPE_BASE = 10000.0
MESH = pl.DeviceIdType.MESH
BF = jnp.bfloat16
F32 = jnp.float32

ROWS = 32
COLS = 512
HEADS = 4
DIM = 2048
FF = 1408
NA = 4
NB = 3


def rms(rows_f, gain):
    inv = lax.rsqrt(jnp.mean(rows_f * rows_f, axis=-1, keepdims=True) + NORM_EPS)
    return (rows_f * inv * gain).astype(BF)


def iota(shape, axis):
    return lax.broadcasted_iota(jnp.int32, shape, axis)


def silu(v):
    return v * jax.nn.sigmoid(v)


def kernel(hid, kc, vc, lens, ids, gts, ga, gf, wq, wkv, wo, sg, su, sd, wg, wu, wd, out,
           hidv, hidc, lensv, idsv, gtsv, gav, gfv, wqkv, wob, kb, vb, abuf, bbuf,
           idsx, cbuf, mbuf, ubuf, xbuf, hbuf, ybuf, rbuf, spart, srecv, obuf,
           sm, wsem, asem, bsem, isend, irecv, csend, crecv, zsend, zrecv, ysend, yrecv, dsend, drecv,
           esend, erecv, rsend, rrecv, ssend, srec, osend, orecv, olocal):
    d = lax.axis_index("dev")
    s = lax.axis_index("side")
    col = pl.ds(pl.multiple_of(s * COLS, COLS), COLS)
    last = s == 3

    small = [(hid, hidv), (hid.at[:, col], hidc), (lens, lensv), (ids.at[0], idsv), (gts.at[0], gtsv), (ga, gav), (gf, gfv)]
    small = [pltpu.make_async_copy(a, b, sm.at[n]) for n, (a, b) in enumerate(small)]
    for c in small:
        c.start()
    vcol = pl.ds(pl.multiple_of(DIM + s * COLS, COLS), COLS)
    big = [(wq.at[0, :, col], wqkv.at[0]), (wkv.at[0, :, col], wqkv.at[1]), (wkv.at[0, :, vcol], wqkv.at[2]),
           (kc.at[0, :, pl.ds(s * HEADS, HEADS)], kb), (vc.at[0, :, pl.ds(s * HEADS, HEADS)], vb), (wo.at[0, :, col], wob)]
    big = [pltpu.make_async_copy(a, b, wsem.at[n]) for n, (a, b) in enumerate(big)]
    for c in big:
        c.start()

    barrier = pltpu.get_barrier_semaphore()
    for k in range(1, 16):
        peer = {"dev": (d + k // 4) % 4, "side": (s + k % 4) % 4}
        pl.semaphore_signal(barrier, inc=1, device_id=peer, device_id_type=MESH)

    ffcol = pl.ds(pl.multiple_of(d * FF, 128), FF)
    shift = jnp.where(last, 1, 0)

    def local_expert(p):
        return 4 * s + p - shift

    def a_copy(p, which, slot):
        src = (wg, wu)[which]
        return pltpu.make_async_copy(src.at[0, local_expert(p)], abuf.at[slot], asem.at[slot])

    def b_copy(p, slot):
        return pltpu.make_async_copy(wd.at[0, local_expert(p)], bbuf.at[slot], bsem.at[slot])

    def first_unit_starts():
        @pl.when(last)
        def _():
            pltpu.make_async_copy(sg.at[0, :, ffcol], abuf.at[0], asem.at[0]).start()
            pltpu.make_async_copy(su.at[0, :, ffcol], abuf.at[1], asem.at[1]).start()
            pltpu.make_async_copy(sd.at[0, pl.ds(pl.multiple_of(d * FF, 128), FF)], bbuf.at[0], bsem.at[0]).start()

        @pl.when(jnp.logical_not(last))
        def _():
            a_copy(0, 0, 0).start()
            a_copy(0, 1, 1).start()
            b_copy(0, 0).start()

    for c in small:
        c.wait()
    normed = rms(hidv[...].astype(F32), gav[...])
    lens_row = lensv[...].astype(F32)
    eye = iota((ROWS, ROWS), 0) == iota((ROWS, ROWS), 1)
    lens_col = jnp.sum(jnp.where(eye, jnp.broadcast_to(lens_row, (ROWS, ROWS)), 0.0), axis=1, keepdims=True)
    lane = iota((ROWS, 128), 1)
    freq = jnp.exp((lane & 63).astype(F32) * (-2.0 * math.log(ROPE_BASE) / 128.0))
    angle = lens_col * freq
    cosine = jnp.cos(angle)
    sine = jnp.where(lane < 64, -jnp.sin(angle), jnp.sin(angle))

    def rope(v):
        return (v * cosine + pltpu.roll(v, 64, axis=1) * sine).astype(BF).astype(F32)

    idf = idsv[...].astype(F32)
    lane32 = iota((ROWS, 128), 1) == d * ROWS + iota((ROWS, 128), 0)
    for j in range(4):
        idsx[d, j:j + 1, :] = jnp.sum(jnp.where(lane32, jnp.broadcast_to(idf[:, j:j + 1], (ROWS, 128)), 0.0), axis=0, keepdims=True)
    for j in range(4):
        rbuf[j, 3, 0] = jnp.zeros((8, 256), BF)

    big[0].wait()
    big[1].wait()
    big[2].wait()
    first_unit_starts()
    a_copy(1, 0, 2).start()
    a_copy(1, 1, 3).start()
    b_copy(1, 1).start()
    b_copy(2, 2).start()
    q_all = jnp.dot(normed, wqkv[0], preferred_element_type=F32).astype(BF).astype(F32)
    k_all = jnp.dot(normed, wqkv[1], preferred_element_type=F32).astype(BF).astype(F32)
    v_all = jnp.dot(normed, wqkv[2], preferred_element_type=F32).astype(BF).astype(F32)
    q_h = [rope(q_all[:, 128 * h:128 * h + 128]) for h in range(HEADS)]
    k_h = [rope(k_all[:, 128 * h:128 * h + 128]) for h in range(HEADS)]
    v_h = [v_all[:, 128 * h:128 * h + 128] for h in range(HEADS)]

    row8 = iota((8, 128), 0)
    big[3].wait()
    parts = []
    for h in range(HEADS):
        for g in range(4):
            q8 = q_h[h][8 * g:8 * g + 8].astype(BF)
            keys = kb[8 * g:8 * g + 8, h].reshape(8 * 128, 128)
            full = lax.dot_general(q8, keys, (((1,), (1,)), ((), ())), preferred_element_type=F32)
            acc = jnp.zeros((8, 128), F32)
            for t in range(8):
                acc = acc + jnp.where(row8 == t, full[:, 128 * t:128 * t + 128], 0.0)
            parts.append(acc)
    scale = 128 ** -0.5
    scores = jnp.concatenate(parts, axis=0) * scale
    q_cat = jnp.concatenate(q_h, axis=0)
    k_cat = jnp.concatenate(k_h, axis=0)
    v_cat = jnp.concatenate(v_h, axis=0)
    lens_cat = jnp.concatenate([lens_col] * HEADS, axis=0)
    scores = jnp.where(iota((128, 128), 1).astype(F32) < lens_cat, scores, -jnp.inf)
    self_score = jnp.sum(q_cat * k_cat, axis=1, keepdims=True) * scale
    peak = jnp.maximum(jnp.max(scores, axis=1, keepdims=True), self_score)
    weights = jnp.exp(scores - peak)
    self_weight = jnp.exp(self_score - peak)
    denom = jnp.sum(weights, axis=1, keepdims=True) + self_weight
    prob = (weights / denom).astype(BF).astype(F32)
    self_prob = (self_weight / denom).astype(BF).astype(F32)
    big[4].wait()
    for h in range(HEADS):
        ctx = []
        for g in range(4):
            n = 4 * h + g
            p8 = prob[8 * n:8 * n + 8]
            wide = jnp.concatenate([jnp.where(row8 == t, p8, 0.0) for t in range(8)], axis=1).astype(BF)
            vals = vb[8 * g:8 * g + 8, h].reshape(8 * 128, 128)
            ctx.append(jnp.dot(wide, vals, preferred_element_type=F32))
        ctx = jnp.concatenate(ctx, axis=0)
        ctx = ctx + self_prob[32 * h:32 * h + 32] * v_cat[32 * h:32 * h + 32]
        cbuf[s, :, 128 * h:128 * h + 128] = ctx.astype(BF)

    pl.semaphore_wait(barrier, 15)
    ccopies = []
    for k in range(1, 4):
        c = pltpu.make_async_remote_copy(cbuf.at[s], cbuf.at[s], csend.at[k], crecv.at[k],
                                         device_id={"side": (s + k) % 4}, device_id_type=MESH)
        c.start()
        ccopies.append(c)
    icopies = []
    for k in range(1, 4):
        c = pltpu.make_async_remote_copy(idsx.at[d], idsx.at[d], isend.at[k], irecv.at[k],
                                         device_id={"dev": (d + k) % 4}, device_id_type=MESH)
        c.start()
        icopies.append(c)
    big[5].wait()
    for c in ccopies:
        c.wait_recv()
    mid = hidc[...].astype(F32)
    attn = jnp.zeros((ROWS, COLS), F32)
    for n in range(4):
        attn = attn + jnp.dot(cbuf[n], wob[COLS * n:COLS * n + COLS], preferred_element_type=F32)
    mid = (mid + attn).astype(BF)
    mbuf[d, s] = mid

    dx = (d, d + 1 - 2 * (d % 2), (d + 2) % 4, 3 - d)
    sx = (s, s + 1 - 2 * (s % 2), (s + 2) % 4, 3 - s)

    def tile_copy(tile, send, recv, peer):
        return pltpu.make_async_remote_copy(tile, tile, send, recv, device_id=peer, device_id_type=MESH)

    zc = [None] + [tile_copy(mbuf.at[d, s], zsend.at[k], zrecv.at[k], {"dev": dx[k]}) for k in range(1, 4)]
    yc = [tile_copy(mbuf.at[dx[q], s], ysend.at[q], yrecv.at[q], {"side": sx[2]}) for q in range(4)]
    dc = [tile_copy(mbuf.at[dx[q], s], dsend.at[q], drecv.at[q], {"side": sx[1]}) for q in range(4)]
    ec = [tile_copy(mbuf.at[dx[q], sx[2]], esend.at[q], erecv.at[q], {"side": sx[1]}) for q in range(4)]
    for k in range(1, 4):
        zc[k].start()
    yc[0].start()
    dc[0].start()

    for c in icopies:
        c.wait_recv()
    id_all = idsx[0] + idsx[1] + idsx[2] + idsx[3]
    r = iota((128, 128), 0)
    t = iota((128, 128), 1)
    unit = r >> 5
    expert = d * 15 + local_expert(unit)
    expert = jnp.where(jnp.logical_and(last, unit == 0), -1, expert).astype(F32)
    hit = jnp.zeros((128, 128), F32)
    for j in range(4):
        hit = hit + jnp.where(jnp.broadcast_to(id_all[j:j + 1], (128, 128)) == expert, 1.0, 0.0)
    earlier = jnp.where(jnp.logical_and(r >> 4 == t >> 4, r < t), 1.0, 0.0).astype(BF)
    rank = jnp.dot(hit.astype(BF), earlier, preferred_element_type=F32)
    place = jnp.logical_and(rank == (r & 1).astype(F32), t >> 4 == 2 * ((r >> 3) & 3) + ((r >> 1) & 1))
    pick = jnp.where(place, hit, 0.0).astype(BF)

    def norm_plane(q):
        dc[q].wait_recv()
        ec[q].wait_recv()
        rows = jnp.concatenate([mbuf[dx[q], n] for n in range(4)], axis=1).astype(F32)
        ubuf[pl.ds(pl.multiple_of(dx[q] * ROWS, ROWS), ROWS), :] = rms(rows, gfv[...])

    yc[0].wait_recv()
    ec[0].start()
    zc[1].wait_recv()
    yc[1].start()
    dc[1].start()
    yc[1].wait_recv()
    ec[1].start()
    zc[2].wait_recv()
    yc[2].start()
    dc[2].start()
    zc[3].wait_recv()
    yc[3].start()
    dc[3].start()
    yc[2].wait_recv()
    ec[2].start()
    yc[3].wait_recv()
    ec[3].start()
    for q in range(4):
        norm_plane(q)
    for n in range(4):
        xs = jnp.dot(pick, ubuf[:, COLS * n:COLS * n + COLS], preferred_element_type=F32).astype(BF)
        xbuf[:, COLS * n:COLS * n + COLS] = xs

    peers = [((d + k // 4) % 4, (s + k % 4) % 4) for k in range(16)]
    low = (iota((32, 256), 0) & 7) < 4
    chunks = [(256 * n, 256) for n in range(5)] + [(1280, 128)]

    def ring_copy(p, k):
        pd, ps = peers[k]
        return pltpu.make_async_remote_copy(ybuf.at[p, pd, ps], rbuf.at[d, s, p], rsend.at[p, k], rrecv.at[p, k],
                                            device_id={"dev": pd, "side": ps}, device_id_type=MESH)

    def part_copy(k):
        pd, ps = peers[k]
        return pltpu.make_async_remote_copy(spart.at[pd, ps], srecv.at[d], ssend.at[k], srec.at[k],
                                            device_id={"dev": pd, "side": ps}, device_id_type=MESH)

    def inner(rows, slot0, slot1, m):
        for off, width in chunks:
            gate = jnp.dot(rows, abuf[slot0, :, off:off + width], preferred_element_type=F32)
            up = jnp.dot(rows, abuf[slot1, :, off:off + width], preferred_element_type=F32)
            hbuf[0:m, off:off + width] = (silu(gate) * up).astype(BF)

    def unit_body(p, carry):
        slot0 = (2 * p) % NA
        slot1 = (2 * p + 1) % NA
        slotb = p % NB
        pltpu.make_async_copy(wg.at[0, 0], abuf.at[slot0], asem.at[slot0]).wait()
        pltpu.make_async_copy(wu.at[0, 0], abuf.at[slot1], asem.at[slot1]).wait()
        is_shared = jnp.logical_and(last, p == 0)

        @pl.when(is_shared)
        def _():
            inner(ubuf[...], slot0, slot1, 128)

        @pl.when(jnp.logical_not(is_shared))
        def _():
            inner(xbuf[pl.ds(pl.multiple_of(p * 32, 32), 32), :], slot0, slot1, 32)

        @pl.when(p < 2)
        def _():
            a_copy(p + 2, 0, slot0).start()
            a_copy(p + 2, 1, slot1).start()

        pltpu.make_async_copy(wd.at[0, 0], bbuf.at[slotb], bsem.at[slotb]).wait()

        @pl.when(is_shared)
        def _():
            rows = hbuf[...]
            for n in range(4):
                for half in range(2):
                    off = COLS * n + 256 * half
                    res = jnp.dot(rows, bbuf[slotb, :, off:off + 256], preferred_element_type=F32)
                    for pd in range(4):
                        spart[pd, n, :, 256 * half:256 * half + 256] = res[32 * pd:32 * pd + 32]
            for k in range(1, 16):
                part_copy(k).start()
            srecv[d] = spart[d, 3]

        @pl.when(jnp.logical_not(is_shared))
        def _():
            rows = hbuf[0:32, :]
            for n in range(4):
                left = jnp.dot(rows, bbuf[slotb, :, COLS * n:COLS * n + 256], preferred_element_type=F32)
                right = jnp.dot(rows, bbuf[slotb, :, COLS * n + 256:COLS * n + 512], preferred_element_type=F32)
                packed = jnp.where(low, left, right)
                for pd in range(4):
                    ybuf[p, pd, n] = packed[8 * pd:8 * pd + 8].astype(BF)
            for k in range(1, 16):
                ring_copy(p, k).start()
            rbuf[d, s, p] = ybuf[p, d, s]

        @pl.when(p < 1)
        def _():
            b_copy(p + 3, slotb).start()

        return carry

    lax.fori_loop(0, 4, unit_body, 0)

    lanes = 512
    l = iota((ROWS, lanes), 1)
    tok = iota((ROWS, lanes), 0)
    lside = (l >> 5) & 3
    lunit = (l >> 3) & 3
    lexp = 15 * (l >> 7) + 4 * lside + lunit - jnp.where(lside == 3, 1, 0)
    lexp = jnp.where(jnp.logical_and(lside == 3, lunit == 0), -1, lexp).astype(F32)
    hits = jnp.zeros((ROWS, lanes), F32)
    gated = jnp.zeros((ROWS, lanes), F32)
    gates = gtsv[...]
    for j in range(4):
        same = jnp.broadcast_to(idf[:, j:j + 1], (ROWS, lanes)) == lexp
        hits = hits + jnp.where(same, 1.0, 0.0)
        gated = gated + jnp.where(same, jnp.broadcast_to(gates[:, j:j + 1], (ROWS, lanes)), 0.0)
    a0 = iota((ROWS, ROWS), 0)
    a1 = iota((ROWS, ROWS), 1)
    before = jnp.where(jnp.logical_and(a0 >> 4 == a1 >> 4, a1 < a0), 1.0, 0.0).astype(BF)
    order = jnp.dot(before, hits.astype(BF), preferred_element_type=F32)
    fits = jnp.logical_and(order == (l & 1).astype(F32), (tok >> 4) == ((l >> 1) & 1))
    gated = jnp.where(fits, gated, 0.0)
    stack = []
    for half in range(2):
        g = jnp.where(((l >> 2) & 1) == half, gated, 0.0)
        for _ in range(3):
            piece = g.astype(BF)
            stack.append(piece)
            g = g - piece.astype(F32)
    stack = jnp.concatenate(stack, axis=0)

    for p in range(4):
        for k in range(1, 16):
            if p == 0:
                from_last = peers_side_is_last(s, k)

                @pl.when(jnp.logical_not(from_last))
                def _():
                    ring_copy(p, k).wait_recv()

                @pl.when(from_last)
                def _():
                    part_copy(k).wait_recv()
            else:
                ring_copy(p, k).wait_recv()
    got = jnp.dot(stack, rbuf[...].reshape(512, 256), preferred_element_type=F32)
    routed = jnp.concatenate([got[0:32] + got[32:64] + got[64:96], got[96:128] + got[128:160] + got[160:192]], axis=1)
    shared = (srecv[0] + srecv[1] + srecv[2] + srecv[3]).astype(BF).astype(F32)
    obuf[...] = (mid.astype(F32) + shared + routed).astype(BF)
    ocopies = [pltpu.make_async_remote_copy(obuf, out.at[:, col], osend.at[k], orecv.at[k],
                                            device_id={"side": (s + k) % 4}, device_id_type=MESH) for k in range(1, 4)]
    for c in ocopies:
        c.start()
    mine = pltpu.make_async_copy(obuf, out.at[:, col], olocal)
    mine.start()

    for c in ccopies + icopies + zc[1:] + yc + dc + ec:
        c.wait_send()

    @pl.when(last)
    def _():
        for k in range(1, 16):
            part_copy(k).wait_send()

    @pl.when(jnp.logical_not(last))
    def _():
        for k in range(1, 16):
            ring_copy(0, k).wait_send()

    for p in range(1, 4):
        for k in range(1, 16):
            ring_copy(p, k).wait_send()
    mine.wait()
    for c in ocopies:
        c.wait()


def peers_side_is_last(s, k):
    return (s + 4 - k % 4) % 4 == 3


def solution(mesh):
    def device_fn(hidden, k_cache, v_cache, cache_lens, expert_ids, route_gates, *weights):
        any_spec = pl.BlockSpec(memory_space=pl.ANY)
        dma = pltpu.SemaphoreType.DMA
        vm = pltpu.VMEM
        return pl.pallas_call(
            kernel,
            out_shape=jax.ShapeDtypeStruct((ROWS, DIM), BF),
            in_specs=[any_spec] * 17,
            out_specs=any_spec,
            scratch_shapes=[
                vm((ROWS, DIM), BF), vm((ROWS, COLS), BF), vm((1, ROWS), jnp.int32), vm((ROWS, 4), jnp.int32),
                vm((ROWS, 4), F32), vm((1, DIM), F32), vm((1, DIM), F32),
                vm((3, DIM, COLS), BF), vm((DIM, COLS), BF),
                vm((ROWS, HEADS, 128, 128), BF), vm((ROWS, HEADS, 128, 128), BF),
                vm((NA, DIM, FF), BF), vm((NB, FF, DIM), BF),
                vm((4, 8, 128), F32), vm((4, ROWS, COLS), BF), vm((4, 4, ROWS, COLS), BF),
                vm((128, DIM), BF), vm((128, DIM), BF), vm((128, FF), BF),
                vm((4, 4, 4, 8, 256), BF), vm((4, 4, 4, 8, 256), BF),
                vm((4, 4, ROWS, COLS), F32), vm((4, ROWS, COLS), F32), vm((ROWS, COLS), BF),
                dma((7,)), dma((6,)), dma((NA,)), dma((NB,)), dma((4,)), dma((4,)), dma((4,)), dma((4,)),
                dma((4,)), dma((4,)), dma((4,)), dma((4,)), dma((4,)), dma((4,)), dma((4,)), dma((4,)),
                dma((4, 16)), dma((4, 16)), dma((16,)), dma((16,)), dma((4,)), dma((4,)), dma,
            ],
            compiler_params=pltpu.CompilerParams(collective_id=0, has_side_effects=True, vmem_limit_bytes=67000000),
            name="moe_decode",
        )(hidden, k_cache, v_cache, cache_lens.reshape(1, ROWS), expert_ids, route_gates, *weights)

    batch = P(("inst", "dev"))
    layer = P(None, ("inst", "dev"))
    expert = P(None, "dev")
    in_specs = (batch, layer, layer, batch, layer, layer) + (P(),) * 8 + (expert,) * 3
    return jax.shard_map(device_fn, mesh=mesh, in_specs=in_specs, out_specs=batch, check_vma=False)
```

```python
import functools
import math

import jax
import jax.numpy as jnp
from jax import lax
from jax.experimental import pallas as pl
from jax.experimental.pallas import tpu as pltpu
from jax.sharding import PartitionSpec as P

NORM_EPS = 1e-6
ROPE_BASE = 10000.0
MESH = pl.DeviceIdType.MESH
BF = jnp.bfloat16
F32 = jnp.float32

ROWS = 32
COLS = 512
HEADS = 4
DIM = 2048
FF = 1408
NA = 5
NB = 4


def rms(rows_f, gain):
    inv = lax.rsqrt(jnp.mean(rows_f * rows_f, axis=-1, keepdims=True) + NORM_EPS)
    return (rows_f * inv * gain).astype(BF)


def iota(shape, axis):
    return lax.broadcasted_iota(jnp.int32, shape, axis)


def silu(v):
    return v * jax.nn.sigmoid(v)


def kernel(hid, kc, vc, lens, ids, gts, ga, gf, wq, wkv, wo, sg, su, sd, wg, wu, wd, out,
           hidv, hidc, lensv, idsv, gtsv, gav, gfv, kb, vb, abuf, bbuf,
           idsx, cbuf, mbuf, ubuf, xbuf, hbuf, ybuf, rbuf, spart, srecv, obuf, stackv,
           sm, wsem, asem, bsem, isend, irecv, csend, crecv, msend, zrecv, yrecv, drecv, erecv,
           rsend, rrecv, ssend, srec, osend, orecv, olocal):
    d = lax.axis_index("dev")
    s = lax.axis_index("side")
    col = pl.ds(pl.multiple_of(s * COLS, COLS), COLS)

    small = [(hid, hidv), (hid.at[:, col], hidc), (lens, lensv), (ids.at[0], idsv), (gts.at[0], gtsv), (ga, gav), (gf, gfv)]
    small = [pltpu.make_async_copy(a, b, sm.at[n]) for n, (a, b) in enumerate(small)]
    for c in small:
        c.start()
    vcol = pl.ds(pl.multiple_of(DIM + s * COLS, COLS), COLS)
    wqv, wkv_k, wkv_v, wob = abuf.at[3, :, 0:512], abuf.at[3, :, 512:1024], abuf.at[4, :, 0:512], abuf.at[4, :, 512:1024]
    big = [(wq.at[0, :, col], wqv), (wkv.at[0, :, col], wkv_k), (wkv.at[0, :, vcol], wkv_v),
           (kc.at[0, :, pl.ds(s * HEADS, HEADS)], kb), (vc.at[0, :, pl.ds(s * HEADS, HEADS)], vb), (wo.at[0, :, col], wob)]
    big = [pltpu.make_async_copy(a, b, wsem.at[n]) for n, (a, b) in enumerate(big)]
    for n in range(3):
        big[n].start()

    barrier = pltpu.get_barrier_semaphore()
    for k in range(1, 16):
        peer = {"dev": (d + k // 4) % 4, "side": (s + k % 4) % 4}
        pl.semaphore_signal(barrier, inc=1, device_id=peer, device_id_type=MESH)

    ffcol = pl.ds(pl.multiple_of(s * FF, 128), FF)

    def local_expert(p):
        return jnp.minimum(4 * s + p, 14)

    def a_copy(n):
        slot = n % NA
        if n < 2:
            return pltpu.make_async_copy((sg, su)[n].at[0, :, ffcol], abuf.at[slot], asem.at[slot])
        return pltpu.make_async_copy((wg, wu)[n % 2].at[0, local_expert(n // 2 - 1)], abuf.at[slot], asem.at[slot])

    def b_copy(n):
        slot = n % NB
        src = sd.at[0, ffcol] if n == 0 else wd.at[0, local_expert(n - 1)]
        return pltpu.make_async_copy(src, bbuf.at[slot], bsem.at[slot])

    for c in small:
        c.wait()
    big[3].start()
    normed = rms(hidv[...].astype(F32), gav[...])
    lens_row = lensv[...].astype(F32)
    eye = iota((ROWS, ROWS), 0) == iota((ROWS, ROWS), 1)
    lens_col = jnp.sum(jnp.where(eye, jnp.broadcast_to(lens_row, (ROWS, ROWS)), 0.0), axis=1, keepdims=True)
    lane = iota((ROWS, 128), 1)
    freq = jnp.exp((lane & 63).astype(F32) * (-2.0 * math.log(ROPE_BASE) / 128.0))
    angle = lens_col * freq
    cosine = jnp.cos(angle)
    sine = jnp.where(lane < 64, -jnp.sin(angle), jnp.sin(angle))

    def rope(v):
        return (v * cosine + pltpu.roll(v, 64, axis=1) * sine).astype(BF).astype(F32)

    idf = idsv[...].astype(F32)
    wide_ids = jnp.concatenate([idf] * 4, axis=1)
    idsx[d, 0:4, :] = jnp.where(iota((4, 128), 1) >> 5 == d, wide_ids, 0.0)
    idsx[d, 4:8, :] = jnp.zeros((4, 128), F32)

    big[0].wait()
    big[4].start()
    q_all = jnp.dot(normed, wqv[...], preferred_element_type=F32).astype(BF).astype(F32)
    big[1].wait()
    big[5].start()
    a_copy(0).start()
    a_copy(1).start()
    b_copy(0).start()
    k_all = jnp.dot(normed, wkv_k[...], preferred_element_type=F32).astype(BF).astype(F32)
    big[2].wait()
    v_all = jnp.dot(normed, wkv_v[...], preferred_element_type=F32).astype(BF).astype(F32)
    a_copy(2).start()
    a_copy(3).start()
    b_copy(1).start()
    b_copy(2).start()
    b_copy(3).start()

    q_h = [rope(q_all[:, 128 * h:128 * h + 128]) for h in range(HEADS)]
    k_h = [rope(k_all[:, 128 * h:128 * h + 128]) for h in range(HEADS)]
    v_h = [v_all[:, 128 * h:128 * h + 128] for h in range(HEADS)]

    row8 = iota((8, 128), 0)
    big[3].wait()
    parts = []
    for h in range(HEADS):
        for g in range(4):
            q8 = q_h[h][8 * g:8 * g + 8].astype(BF)
            keys = kb[8 * g:8 * g + 8, h].reshape(8 * 128, 128)
            full = lax.dot_general(q8, keys, (((1,), (1,)), ((), ())), preferred_element_type=F32)
            acc = jnp.zeros((8, 128), F32)
            for t in range(8):
                acc = acc + jnp.where(row8 == t, full[:, 128 * t:128 * t + 128], 0.0)
            parts.append(acc)
    scale = 128 ** -0.5
    scores = jnp.concatenate(parts, axis=0) * scale
    q_cat = jnp.concatenate(q_h, axis=0)
    k_cat = jnp.concatenate(k_h, axis=0)
    v_cat = jnp.concatenate(v_h, axis=0)
    lens_cat = jnp.concatenate([lens_col] * HEADS, axis=0)
    scores = jnp.where(iota((128, 128), 1).astype(F32) < lens_cat, scores, -jnp.inf)
    self_score = jnp.sum(q_cat * k_cat, axis=1, keepdims=True) * scale
    peak = jnp.maximum(jnp.max(scores, axis=1, keepdims=True), self_score)
    weights = jnp.exp(scores - peak)
    self_weight = jnp.exp(self_score - peak)
    denom = jnp.sum(weights, axis=1, keepdims=True) + self_weight
    prob = (weights / denom).astype(BF).astype(F32)
    self_prob = (self_weight / denom).astype(BF).astype(F32)
    big[4].wait()
    for h in range(HEADS):
        ctx = []
        for g in range(4):
            n = 4 * h + g
            p8 = prob[8 * n:8 * n + 8]
            wide = jnp.concatenate([jnp.where(row8 == t, p8, 0.0) for t in range(8)], axis=1).astype(BF)
            vals = vb[8 * g:8 * g + 8, h].reshape(8 * 128, 128)
            ctx.append(jnp.dot(wide, vals, preferred_element_type=F32))
        ctx = jnp.concatenate(ctx, axis=0)
        ctx = ctx + self_prob[32 * h:32 * h + 32] * v_cat[32 * h:32 * h + 32]
        cbuf[s, :, 128 * h:128 * h + 128] = ctx.astype(BF)

    pl.semaphore_wait(barrier, 15)
    ccopies = []
    for k in range(1, 4):
        c = pltpu.make_async_remote_copy(cbuf.at[s], cbuf.at[s], csend, crecv,
                                         device_id={"side": (s + k) % 4}, device_id_type=MESH)
        c.start()
        ccopies.append(c)
    icopies = []
    for k in range(1, 4):
        c = pltpu.make_async_remote_copy(idsx.at[d], idsx.at[d], isend, irecv,
                                         device_id={"dev": (d + k) % 4}, device_id_type=MESH)
        c.start()
        icopies.append(c)

    lanes = 512
    l = iota((ROWS, lanes), 1)
    tok = iota((ROWS, lanes), 0)
    lside = (l >> 5) & 3
    lunit = (l >> 3) & 3
    lexp = 4 * lside + lunit
    lexp = jnp.where(lexp < 15, 15 * (l >> 7) + lexp, -1).astype(F32)
    hits = jnp.zeros((ROWS, lanes), F32)
    gated = jnp.zeros((ROWS, lanes), F32)
    gates = gtsv[...]

    def column(row):
        return jnp.sum(jnp.where(eye, jnp.broadcast_to(row, (ROWS, ROWS)), 0.0), axis=1, keepdims=True)

    for j in range(4):
        same = jnp.broadcast_to(column(idf[j:j + 1]), (ROWS, lanes)) == lexp
        hits = hits + jnp.where(same, 1.0, 0.0)
        gated = gated + jnp.where(same, jnp.broadcast_to(column(gates[j:j + 1]), (ROWS, lanes)), 0.0)
    a0 = iota((ROWS, ROWS), 0)
    a1 = iota((ROWS, ROWS), 1)
    before = jnp.where(jnp.logical_and(a0 >> 4 == a1 >> 4, a1 < a0), 1.0, 0.0).astype(BF)
    order = jnp.dot(before, hits.astype(BF), preferred_element_type=F32)
    fits = jnp.logical_and(order == (l & 1).astype(F32), (tok >> 4) == ((l >> 1) & 1))
    gated = jnp.where(fits, gated, 0.0)
    stack = []
    for half in range(2):
        g = jnp.where(((l >> 2) & 1) == half, gated, 0.0)
        for _ in range(3):
            piece = g.astype(BF)
            stack.append(piece)
            g = g - piece.astype(F32)
    stackv[...] = jnp.concatenate(stack, axis=0)

    big[5].wait()
    pltpu.make_async_copy(cbuf.at[0:3], cbuf.at[0:3], crecv).wait()
    mid = hidc[...].astype(F32)
    attn = jnp.zeros((ROWS, COLS), F32)
    for n in range(4):
        attn = attn + jnp.dot(cbuf[n], wob[COLS * n:COLS * n + COLS, :], preferred_element_type=F32)
    mid = (mid + attn).astype(BF)
    mbuf[4 * d + s] = mid
    a_copy(4).start()

    dx = (d, d + 1 - 2 * (d % 2), (d + 2) % 4, 3 - d)
    sx = (s, s + 1 - 2 * (s % 2), (s + 2) % 4, 3 - s)

    def tile_copy(plane, side, recv, peer):
        tile = mbuf.at[4 * plane + side]
        return pltpu.make_async_remote_copy(tile, tile, msend, recv, device_id=peer, device_id_type=MESH)

    zc = [None] + [tile_copy(d, s, zrecv.at[k - 1], {"dev": dx[k]}) for k in range(1, 4)]
    yc = [tile_copy(dx[q], s, yrecv.at[q], {"side": sx[2]}) for q in range(4)]
    dc = [tile_copy(dx[q], s, drecv.at[q], {"side": sx[1]}) for q in range(4)]
    ec = [tile_copy(dx[q], sx[2], erecv.at[q], {"side": sx[1]}) for q in range(4)]

    def from_z(k):
        zc[k].wait_recv()
        yc[k].start()
        dc[k].start()

    def from_y(q):
        yc[q].wait_recv()
        ec[q].start()

    def norm_plane(q):
        dc[q].wait_recv()
        ec[q].wait_recv()
        rows = jnp.concatenate([mbuf[4 * dx[q] + n] for n in range(4)], axis=1).astype(F32)
        u = rms(rows, gfv[...])
        ubuf[pl.ds(pl.multiple_of(dx[q] * ROWS, ROWS), ROWS), :] = u


    for k in range(1, 4):
        zc[k].start()
    yc[0].start()
    dc[0].start()

    chunks = [(256 * n, 256) for n in range(5)] + [(1280, 128)]

    def inner(rows, slot0, slot1, part):
        for off, width in part:
            gate = jnp.dot(rows, abuf[slot0, :, off:off + width], preferred_element_type=F32)
            up = jnp.dot(rows, abuf[slot1, :, off:off + width], preferred_element_type=F32)
            hbuf[:, off:off + width] = (silu(gate) * up).astype(BF)

    def shared_down(n):
        spart[n] = jnp.dot(hbuf[...], bbuf[0, :, COLS * n:COLS * n + COLS], preferred_element_type=F32)

    from_y(0)
    pltpu.make_async_copy(idsx.at[0:3], idsx.at[0:3], irecv).wait()
    id_all = idsx[0] + idsx[1] + idsx[2] + idsx[3]
    r = iota((128, 128), 0)
    t = iota((128, 128), 1)
    unit = r >> 5
    expert = 4 * s + unit
    expert = jnp.where(expert < 15, d * 15 + expert, -1).astype(F32)
    hit = jnp.zeros((128, 128), F32)
    for j in range(4):
        hit = hit + jnp.where(jnp.broadcast_to(id_all[j:j + 1], (128, 128)) == expert, 1.0, 0.0)
    earlier = jnp.where(jnp.logical_and(r >> 4 == t >> 4, r < t), 1.0, 0.0).astype(BF)
    rank = jnp.dot(hit.astype(BF), earlier, preferred_element_type=F32)
    place = jnp.logical_and(rank == (r & 1).astype(F32), t >> 4 == 2 * ((r >> 3) & 3) + ((r >> 1) & 1))
    pick = jnp.where(place, hit, 0.0).astype(BF)

    from_z(1)
    norm_plane(0)
    mine_rows = pl.ds(pl.multiple_of(d * ROWS, ROWS), ROWS)
    a_copy(0).wait()
    a_copy(1).wait()
    inner(ubuf[mine_rows, :], 0, 1, chunks[0:3])
    from_y(1)
    from_z(2)
    inner(ubuf[mine_rows, :], 0, 1, chunks[3:6])
    a_copy(5).start()
    a_copy(6).start()
    b_copy(0).wait()
    from_z(3)
    shared_down(0)
    shared_down(1)
    from_y(2)
    shared_down(2)
    shared_down(3)
    b_copy(4).start()
    from_y(3)
    for q in range(1, 4):
        norm_plane(q)
    scopies = []
    for k in range(1, 4):
        peer = (s + k) % 4
        c = pltpu.make_async_remote_copy(spart.at[peer], srecv.at[s], ssend, srec, device_id={"side": peer}, device_id_type=MESH)
        c.start()
        scopies.append(c)
    for n in range(4):
        xs = jnp.dot(pick, ubuf[:, COLS * n:COLS * n + COLS], preferred_element_type=F32).astype(BF)
        xbuf[:, COLS * n:COLS * n + COLS] = xs

    peers = [((d + k // 4) % 4, (s + k % 4) % 4) for k in range(16)]
    low = (iota((32, 256), 0) & 7) < 4

    def row_copy(p, k):
        pd, ps = peers[k]
        return pltpu.make_async_remote_copy(ybuf.at[4 * pd + ps, p], rbuf.at[4 * d + s, p], rsend, rrecv,
                                            device_id={"dev": pd, "side": ps}, device_id_type=MESH)

    def unit_body(p, carry):
        slot0 = (2 * p + 2) % NA
        slot1 = (2 * p + 3) % NA
        slotb = (p + 1) % NB
        pltpu.make_async_copy(wg.at[0, 0], abuf.at[slot0], asem.at[slot0]).wait()
        pltpu.make_async_copy(wu.at[0, 0], abuf.at[slot1], asem.at[slot1]).wait()
        inner(xbuf[pl.ds(pl.multiple_of(p * 32, 32), 32), :], slot0, slot1, chunks)

        @pl.when(p == 0)
        def _():
            a_copy(7).start()
            a_copy(8).start()

        @pl.when(p == 1)
        def _():
            a_copy(9).start()

        pltpu.make_async_copy(wd.at[0, 0], bbuf.at[slotb], bsem.at[slotb]).wait()
        rows = hbuf[...]
        for n in range(4):
            left = jnp.dot(rows, bbuf[slotb, :, COLS * n:COLS * n + 256], preferred_element_type=F32)
            right = jnp.dot(rows, bbuf[slotb, :, COLS * n + 256:COLS * n + 512], preferred_element_type=F32)
            packed = jnp.where(low, left, right)
            for pd in range(4):
                ybuf[4 * pd + n, p] = packed[8 * pd:8 * pd + 8].astype(BF)
        for k in range(1, 16):
            row_copy(p, k).start()
        return carry

    lax.fori_loop(0, 4, unit_body, 0)

    rbuf[4 * d + s] = ybuf[4 * d + s]
    srecv[s] = spart[s]
    pltpu.make_async_copy(spart.at[0:3], spart.at[0:3], srec).wait()
    shared = (srecv[0] + srecv[1] + srecv[2] + srecv[3]).astype(BF).astype(F32)
    pltpu.make_async_copy(ybuf.at[0:15], ybuf.at[0:15], rrecv).wait()
    got = jnp.dot(stackv[...], rbuf[...].reshape(512, 256), preferred_element_type=F32)
    routed = jnp.concatenate([got[0:32] + got[32:64] + got[64:96], got[96:128] + got[128:160] + got[160:192]], axis=1)
    obuf[...] = (mid.astype(F32) + shared + routed).astype(BF)
    ocopies = [pltpu.make_async_remote_copy(obuf, out.at[:, col], osend, orecv,
                                            device_id={"side": (s + k) % 4}, device_id_type=MESH) for k in range(1, 4)]
    for c in ocopies:
        c.start()
    mine = pltpu.make_async_copy(obuf, out.at[:, col], olocal)
    mine.start()

    pltpu.make_async_copy(cbuf.at[0:3], cbuf.at[0:3], csend).wait()
    pltpu.make_async_copy(idsx.at[0:3], idsx.at[0:3], isend).wait()
    pltpu.make_async_copy(mbuf.at[0:15], mbuf.at[0:15], msend).wait()
    pltpu.make_async_copy(spart.at[0:3], spart.at[0:3], ssend).wait()
    pltpu.make_async_copy(ybuf.at[0:15], ybuf.at[0:15], rsend).wait()
    pltpu.make_async_copy(cbuf.at[0:3], cbuf.at[0:3], osend).wait()
    mine.wait()
    pltpu.make_async_copy(cbuf.at[0:3], cbuf.at[0:3], orecv).wait()


def solution(mesh):
    def device_fn(hidden, k_cache, v_cache, cache_lens, expert_ids, route_gates, *weights):
        any_spec = pl.BlockSpec(memory_space=pl.ANY)
        dma = pltpu.SemaphoreType.DMA
        vm = pltpu.VMEM
        return pl.pallas_call(
            kernel,
            out_shape=jax.ShapeDtypeStruct((ROWS, DIM), BF),
            in_specs=[any_spec] * 17,
            out_specs=any_spec,
            scratch_shapes=[
                vm((ROWS, DIM), BF), vm((ROWS, COLS), BF), vm((1, ROWS), jnp.int32), vm((4, ROWS), jnp.int32),
                vm((4, ROWS), F32), vm((1, DIM), F32), vm((1, DIM), F32),
                vm((ROWS, HEADS, 128, 128), BF), vm((ROWS, HEADS, 128, 128), BF),
                vm((NA, DIM, FF), BF), vm((NB, FF, DIM), BF),
                vm((4, 8, 128), F32), vm((4, ROWS, COLS), BF), vm((16, ROWS, COLS), BF),
                vm((128, DIM), BF), vm((128, DIM), BF), vm((ROWS, FF), BF),
                vm((16, 4, 8, 256), BF), vm((16, 4, 8, 256), BF),
                vm((4, ROWS, COLS), F32), vm((4, ROWS, COLS), F32), vm((ROWS, COLS), BF), vm((192, 512), BF),
                dma((7,)), dma((6,)), dma((NA,)), dma((NB,)), dma, dma, dma, dma, dma, dma((3,)), dma((4,)), dma((4,)), dma((4,)),
                dma, dma, dma, dma, dma, dma, dma,
            ],
            compiler_params=pltpu.CompilerParams(collective_id=0, has_side_effects=True, vmem_limit_bytes=67000000),
            name="moe_decode",
        )(hidden, k_cache, v_cache, cache_lens.reshape(1, ROWS), jnp.swapaxes(expert_ids, 1, 2),
          jnp.swapaxes(route_gates, 1, 2), *weights)

    batch = P(("inst", "dev"))
    layer = P(None, ("inst", "dev"))
    expert = P(None, "dev")
    in_specs = (batch, layer, layer, batch, layer, layer) + (P(),) * 8 + (expert,) * 3
    return jax.shard_map(device_fn, mesh=mesh, in_specs=in_specs, out_specs=batch, check_vma=False)
```

```python
import functools
import math

import jax
import jax.numpy as jnp
from jax import lax
from jax.experimental import pallas as pl
from jax.experimental.pallas import tpu as pltpu
from jax.sharding import PartitionSpec as P

NORM_EPS = 1e-6
ROPE_BASE = 10000.0
MESH = pl.DeviceIdType.MESH
BF = jnp.bfloat16
F32 = jnp.float32

ROWS = 32
COLS = 512
HEADS = 4
DIM = 2048
FF = 1408
SPLIT = 1024
TAIL = 1152
NA = 5
NB = 4


def rms(rows_f, gain):
    inv = lax.rsqrt(jnp.mean(rows_f * rows_f, axis=-1, keepdims=True) + NORM_EPS)
    return (rows_f * inv * gain).astype(BF)


class Load:
    def __init__(self, src, dst, sem, pieces=4):
        rows = dst.shape[0] // pieces
        self.whole = (src, dst, sem)
        self.pieces = [(src.at[rows * n:rows * n + rows], dst.at[rows * n:rows * n + rows], sem) for n in range(pieces)]

    def start(self):
        for c in self.pieces:
            pltpu.make_async_copy(*c).start()

    def wait(self):
        pltpu.make_async_copy(*self.whole).wait()


def arrived(ref, blocks, sem):
    pltpu.make_async_copy(ref.at[:blocks], ref.at[:blocks], sem).wait()


def span(n, width):
    return slice(width * n, width * n + width)


def flag(condition):
    return jnp.where(condition, 1.0, 0.0)


def row_id(shape):
    return lax.broadcasted_iota(jnp.int32, shape, 0)


def col_id(shape):
    return lax.broadcasted_iota(jnp.int32, shape, 1)


def silu(v):
    return v * jax.nn.sigmoid(v)


def kernel(hid, kc, vc, lens, ids, gts, ga, gf, wq, wkv, wo, sg, su, sd, wg, wu, wd, out,
           hidv, hidc, lensv, idsv, gtsv, gav, gfv, kb, vb, abuf, bbuf,
           idsx, cbuf, mbuf, ubuf, xbuf, hbuf, ybuf, rbuf, spart, srecv, stackv,
           sm, wsem, asem, bsem, isend, irecv, csend, crecv, msend, zrecv, yrecv, drecv, erecv,
           rsend, rrecv, ssend, srec, osend, orecv):
    d = lax.axis_index("dev")
    s = lax.axis_index("side")
    col = pl.ds(pl.multiple_of(s * COLS, COLS), COLS)

    kc, vc, ids, gts, wq, wkv, wo, sg, su, sd, wg, wu, wd = (ref.at[0] for ref in (kc, vc, ids, gts, wq, wkv, wo, sg, su, sd, wg, wu, wd))
    small = [(hid, hidv), (hid.at[:, col], hidc), (lens, lensv), (ids, idsv), (gts, gtsv), (ga, gav), (gf, gfv)]
    small = [pltpu.make_async_copy(a, b, sm.at[n]) for n, (a, b) in enumerate(small)]
    for c in small:
        c.start()
    vcol = pl.ds(pl.multiple_of(DIM + s * COLS, COLS), COLS)
    wqv, wkv_k, wkv_v, wob = abuf.at[3, :, 0:512], abuf.at[3, :, 512:1024], abuf.at[4, :, 0:512], abuf.at[4, :, 512:1024]
    big = [(wq.at[:, col], wqv), (wkv.at[:, col], wkv_k), (wkv.at[:, vcol], wkv_v),
           (kc.at[:, pl.ds(s * HEADS, 2)], kb.at[:, 0:2]), (vc.at[:, pl.ds(s * HEADS, 2)], vb.at[:, 0:2]), (wo.at[:, col], wob),
           (kc.at[:, pl.ds(s * HEADS + 2, 2)], kb.at[:, 2:4]), (vc.at[:, pl.ds(s * HEADS + 2, 2)], vb.at[:, 2:4])]
    big = [pltpu.make_async_copy(a, b, wsem.at[n]) for n, (a, b) in enumerate(big)]
    for n in range(3):
        big[n].start()

    barrier = pltpu.get_barrier_semaphore()
    for k in range(1, 16):
        peer = {"dev": (d + k // 4) % 4, "side": (s + k % 4) % 4}
        pl.semaphore_signal(barrier, inc=1, device_id=peer, device_id_type=MESH)

    last = s == 3
    front = jnp.logical_not(last)
    shift = jnp.where(last, 1, 0)
    head = pl.ds(pl.multiple_of(s * SPLIT, SPLIT), SPLIT)
    body = pl.ds(3 * SPLIT, FF)
    rest = pl.ds(3 * SPLIT + FF, TAIL)

    def local_expert(p):
        return 4 * s + p - shift

    def a_expert(n):
        slot = n % NA
        return Load((wg, wu)[n % 2].at[local_expert(n // 2 - 1)], abuf.at[slot], asem.at[slot])

    def a_shared(n, part):
        width = {SPLIT: head, FF: body, TAIL: rest}[part]
        return Load((sg, su)[n % 2].at[:, width], abuf.at[n, :, 0:part], asem.at[n])

    def b_expert(n):
        slot = n % NB
        return Load(wd.at[local_expert(n - 1)], bbuf.at[slot], bsem.at[slot])

    def b_shared(n, part):
        width = {SPLIT: head, FF: body, TAIL: rest}[part]
        return Load(sd.at[width], bbuf.at[n, 0:part], bsem.at[n])

    for n in range(16):
        ybuf[n, 0] = jnp.zeros((8, 256), BF)
    for c in small:
        c.wait()
    big[3].start()
    big[6].start()
    normed = rms(hidv[...].astype(F32), gav[...])
    lens_row = lensv[...].astype(F32)
    eye = row_id((ROWS, ROWS)) == col_id((ROWS, ROWS))
    lens_col = jnp.sum(jnp.where(eye, jnp.broadcast_to(lens_row, (ROWS, ROWS)), 0.0), axis=1, keepdims=True)
    lane = col_id((ROWS, 128))
    freq = jnp.exp((lane & 63).astype(F32) * (-2.0 * math.log(ROPE_BASE) / 128.0))
    angle = lens_col * freq
    cosine = jnp.cos(angle)
    sine = jnp.where(lane < 64, -jnp.sin(angle), jnp.sin(angle))

    def rope(v):
        return (v * cosine + pltpu.roll(v, 64, axis=1) * sine).astype(BF).astype(F32)

    idf = idsv[...].astype(F32)
    wide_ids = jnp.concatenate([idf] * 4, axis=1)
    idsx[d, 0:4, :] = jnp.where(col_id((4, 128)) >> 5 == d, wide_ids, 0.0)
    idsx[d, 4:8, :] = jnp.zeros((4, 128), F32)

    big[0].wait()
    big[4].start()
    big[7].start()
    q_all = jnp.dot(normed, wqv[...], preferred_element_type=F32).astype(BF).astype(F32)
    big[1].wait()
    big[5].start()

    @pl.when(last)
    def _():
        a_shared(0, FF).start()
        a_shared(1, FF).start()
        b_shared(0, FF).start()

    @pl.when(front)
    def _():
        a_shared(0, SPLIT).start()
        a_shared(1, SPLIT).start()
        b_shared(0, SPLIT).start()

    k_all = jnp.dot(normed, wkv_k[...], preferred_element_type=F32).astype(BF).astype(F32)
    big[2].wait()
    v_all = jnp.dot(normed, wkv_v[...], preferred_element_type=F32).astype(BF).astype(F32)

    @pl.when(last)
    def _():
        a_shared(2, TAIL).start()
        a_shared(3, TAIL).start()
        b_shared(1, TAIL).start()

    @pl.when(front)
    def _():
        a_expert(2).start()
        a_expert(3).start()
        b_expert(1).start()

    b_expert(2).start()
    b_expert(3).start()

    q_h = [rope(q_all[:, span(h, 128)]) for h in range(HEADS)]
    k_h = [rope(k_all[:, span(h, 128)]) for h in range(HEADS)]
    v_h = [v_all[:, span(h, 128)] for h in range(HEADS)]

    row8 = row_id((8, 128))
    big[3].wait()
    parts = []
    for h in range(HEADS):
        if h == 2:
            big[6].wait()
        for g in range(4):
            q8 = q_h[h][span(g, 8)].astype(BF)
            keys = kb[span(g, 8), h].reshape(8 * 128, 128)
            full = lax.dot_general(q8, keys, (((1,), (1,)), ((), ())), preferred_element_type=F32)
            acc = jnp.zeros((8, 128), F32)
            for t in range(8):
                acc = acc + jnp.where(row8 == t, full[:, span(t, 128)], 0.0)
            parts.append(acc)
    scale = 128 ** -0.5
    scores = jnp.concatenate(parts, axis=0) * scale
    q_cat = jnp.concatenate(q_h, axis=0)
    k_cat = jnp.concatenate(k_h, axis=0)
    v_cat = jnp.concatenate(v_h, axis=0)
    lens_cat = jnp.concatenate([lens_col] * HEADS, axis=0)
    scores = jnp.where(col_id((128, 128)).astype(F32) < lens_cat, scores, -jnp.inf)
    self_score = jnp.sum(q_cat * k_cat, axis=1, keepdims=True) * scale
    peak = jnp.maximum(jnp.max(scores, axis=1, keepdims=True), self_score)
    weights = jnp.exp(scores - peak)
    self_weight = jnp.exp(self_score - peak)
    denom = jnp.sum(weights, axis=1, keepdims=True) + self_weight
    prob = (weights / denom).astype(BF).astype(F32)
    self_prob = (self_weight / denom).astype(BF).astype(F32)
    big[4].wait()
    for h in range(HEADS):
        if h == 2:
            big[7].wait()
        ctx = []
        for g in range(4):
            n = 4 * h + g
            p8 = prob[span(n, 8)]
            wide = jnp.concatenate([jnp.where(row8 == t, p8, 0.0) for t in range(8)], axis=1).astype(BF)
            vals = vb[span(g, 8), h].reshape(8 * 128, 128)
            ctx.append(jnp.dot(wide, vals, preferred_element_type=F32))
        ctx = jnp.concatenate(ctx, axis=0)
        ctx = ctx + self_prob[span(h, 32)] * v_cat[span(h, 32)]
        cbuf[s, :, span(h, 128)] = ctx.astype(BF)

    pl.semaphore_wait(barrier, 15)
    ccopies = []
    for k in range(1, 4):
        c = pltpu.make_async_remote_copy(cbuf.at[s], cbuf.at[s], csend, crecv,
                                         device_id={"side": (s + k) % 4}, device_id_type=MESH)
        c.start()
        ccopies.append(c)
    icopies = []
    for k in range(1, 4):
        c = pltpu.make_async_remote_copy(idsx.at[d], idsx.at[d], isend, irecv,
                                         device_id={"dev": (d + k) % 4}, device_id_type=MESH)
        c.start()
        icopies.append(c)

    lanes = 512
    l = col_id((ROWS, lanes))
    tok = row_id((ROWS, lanes))
    lside = (l >> 5) & 3
    lunit = (l >> 3) & 3
    lexp = 15 * (l >> 7) + 4 * lside + lunit - jnp.where(lside == 3, 1, 0)
    lexp = jnp.where(jnp.logical_and(lside == 3, lunit == 0), -1, lexp).astype(F32)
    hits = jnp.zeros((ROWS, lanes), F32)
    gated = jnp.zeros((ROWS, lanes), F32)
    gates = gtsv[...]

    def column(row):
        return jnp.sum(jnp.where(eye, jnp.broadcast_to(row, (ROWS, ROWS)), 0.0), axis=1, keepdims=True)

    for j in range(4):
        same = jnp.broadcast_to(column(idf[j:j + 1]), (ROWS, lanes)) == lexp
        hits = hits + flag(same)
        gated = gated + jnp.where(same, jnp.broadcast_to(column(gates[j:j + 1]), (ROWS, lanes)), 0.0)
    a0 = row_id((ROWS, ROWS))
    a1 = col_id((ROWS, ROWS))
    before = flag(jnp.logical_and(a0 >> 4 == a1 >> 4, a1 < a0)).astype(BF)
    order = jnp.dot(before, hits.astype(BF), preferred_element_type=F32)
    fits = jnp.logical_and(order == (l & 1).astype(F32), (tok >> 4) == ((l >> 1) & 1))
    gated = jnp.where(fits, gated, 0.0)
    stack = []
    for half in range(2):
        g = jnp.where(((l >> 2) & 1) == half, gated, 0.0)
        for _ in range(3):
            piece = g.astype(BF)
            stack.append(piece)
            g = g - piece.astype(F32)
    stackv[...] = jnp.concatenate(stack, axis=0)

    big[5].wait()
    arrived(cbuf, 3, crecv)
    mid = hidc[...].astype(F32)
    attn = jnp.zeros((ROWS, COLS), F32)
    for n in range(4):
        attn = attn + jnp.dot(cbuf[n], wob[span(n, COLS), :], preferred_element_type=F32)
    mid = (mid + attn).astype(BF)
    mbuf[4 * d + s] = mid
    a_expert(4).start()

    dx = (d, d + 1 - 2 * (d % 2), (d + 2) % 4, 3 - d)
    sx = (s, s + 1 - 2 * (s % 2), (s + 2) % 4, 3 - s)

    def tile_copy(plane, side, recv, peer):
        tile = mbuf.at[4 * plane + side]
        return pltpu.make_async_remote_copy(tile, tile, msend, recv, device_id=peer, device_id_type=MESH)

    inside = jnp.logical_or(d == 1, d == 2)
    code = (0, 1, jnp.where(inside, 3, 2), jnp.where(inside, 2, 3))
    near = (d, dx[1], jnp.where(inside, dx[3], dx[2]), jnp.where(inside, dx[2], dx[3]))
    zc = [None] + [tile_copy(d, s, zrecv.at[code[k]], {"dev": near[k]}) for k in range(1, 4)]
    yc = [tile_copy(near[q], s, yrecv.at[q], {"side": sx[2]}) for q in range(4)]
    dc = [tile_copy(near[q], s, drecv.at[q], {"side": sx[1]}) for q in range(4)]
    ec = [tile_copy(near[q], sx[2], erecv.at[q], {"side": sx[1]}) for q in range(4)]

    def from_z(k):
        zc[k].wait_recv()
        yc[k].start()
        dc[k].start()

    def from_y(q):
        yc[q].wait_recv()
        ec[q].start()

    def norm_plane(q):
        dc[q].wait_recv()
        ec[q].wait_recv()
        rows = jnp.concatenate([mbuf[4 * near[q] + n] for n in range(4)], axis=1).astype(F32)
        u = rms(rows, gfv[...])
        ubuf[pl.ds(pl.multiple_of(near[q] * ROWS, ROWS), ROWS), :] = u


    for k in range(1, 4):
        zc[k].start()
    yc[0].start()
    dc[0].start()

    chunks = [(256 * n, 256) for n in range(5)] + [(1280, 128)]

    def inner(rows, slot0, slot1, part):
        for off, width in part:
            gate = jnp.dot(rows, abuf[slot0, :, off:off + width], preferred_element_type=F32)
            up = jnp.dot(rows, abuf[slot1, :, off:off + width], preferred_element_type=F32)
            hbuf[:, off:off + width] = (silu(gate) * up).astype(BF)

    def shared_down(n):
        cols = slice(COLS * n, COLS * n + COLS)
        spart[n] = jnp.dot(hbuf[:, 0:SPLIT], bbuf[0, 0:SPLIT, cols], preferred_element_type=F32)

        @pl.when(last)
        def _():
            spart[n] = spart[n] + jnp.dot(hbuf[:, SPLIT:FF], bbuf[0, SPLIT:FF, cols], preferred_element_type=F32)


    from_y(0)
    arrived(idsx, 3, irecv)
    id_all = idsx[0] + idsx[1] + idsx[2] + idsx[3]
    r = row_id((64, 128))
    t = col_id((64, 128))
    unit = r >> 4
    expert = d * 15 + local_expert(unit)
    expert = jnp.where(jnp.logical_and(last, unit == 0), -1, expert).astype(F32)
    hit = jnp.zeros((64, 128), F32)
    for j in range(4):
        hit = hit + flag(jnp.broadcast_to(id_all[j:j + 1], (64, 128)) == expert)
    t0 = row_id((128, 128))
    t1 = col_id((128, 128))
    earlier = flag(jnp.logical_and(t0 >> 4 == t1 >> 4, t0 < t1)).astype(BF)
    rank = jnp.dot(hit.astype(BF), earlier, preferred_element_type=F32)
    place = jnp.logical_and(rank == (r & 1).astype(F32), t >> 4 == 2 * ((r >> 2) & 3) + ((r >> 1) & 1))
    pick = jnp.where(place, hit, 0.0).astype(BF)

    from_z(1)
    norm_plane(0)
    mine_rows = pl.ds(pl.multiple_of(d * ROWS, ROWS), ROWS)

    @pl.when(last)
    def _():
        a_shared(0, FF).wait()
        a_shared(1, FF).wait()

    @pl.when(front)
    def _():
        a_shared(0, SPLIT).wait()
        a_shared(1, SPLIT).wait()

    inner(ubuf[mine_rows, :], 0, 1, chunks[0:2])
    from_z(2)
    inner(ubuf[mine_rows, :], 0, 1, chunks[2:4])
    from_z(3)

    @pl.when(last)
    def _():
        inner(ubuf[mine_rows, :], 0, 1, chunks[4:6])

    a_expert(5).start()
    a_expert(6).start()

    @pl.when(last)
    def _():
        b_shared(0, FF).wait()

    @pl.when(front)
    def _():
        b_shared(0, SPLIT).wait()

    from_y(1)
    shared_down(0)
    from_y(2)
    shared_down(1)
    shared_down(2)
    from_y(3)
    shared_down(3)
    @pl.when(last)
    def _():
        a_shared(2, TAIL).wait()
        a_shared(3, TAIL).wait()
        inner(ubuf[mine_rows, :], 2, 3, chunks[0:4] + [(SPLIT, 128)])
        b_shared(1, TAIL).wait()
        for n in range(4):
            spart[n] = spart[n] + jnp.dot(hbuf[:, 0:TAIL], bbuf[1, 0:TAIL, span(n, COLS)], preferred_element_type=F32)

    for q in range(1, 4):
        norm_plane(q)
    for k in range(1, 4):
        peer = (s + k) % 4
        pltpu.make_async_remote_copy(spart.at[peer], srecv.at[s], ssend, srec, device_id={"side": peer}, device_id_type=MESH).start()
    for n in range(4):
        xs = jnp.dot(pick, ubuf[:, span(n, COLS)], preferred_element_type=F32).astype(BF)
        xbuf[:, span(n, COLS)] = xs

    low = row_id((8, 256)) < 4

    def row_copy(p, pd, ps):
        return pltpu.make_async_remote_copy(ybuf.at[4 * pd + ps, p], rbuf.at[4 * d + s, p], rsend, rrecv,
                                            device_id={"dev": pd, "side": ps}, device_id_type=MESH)

    def send_rows(p, hop, first):
        for q in (2, 3, 1, 0):
            for side in ((s + 1) % 2, s % 2):
                if hop or q:
                    row_copy(p, dx[q], first + side).start()
        if not hop:
            row_copy(p, d, sx[1]).start()

    def unit_body(p, carry):
        slot0 = (2 * p + 2) % NA
        slot1 = (2 * p + 3) % NA
        slotb = (p + 1) % NB
        is_rest = jnp.logical_and(last, p == 0)

        @pl.when(jnp.logical_not(is_rest))
        def _():
            pltpu.make_async_copy(wg.at[0], abuf.at[slot0], asem.at[slot0]).wait()
            pltpu.make_async_copy(wu.at[0], abuf.at[slot1], asem.at[slot1]).wait()

            rows = xbuf[pl.ds(pl.multiple_of(p * 16, 16), 16), :]
            gate = jnp.dot(rows, abuf[slot0], preferred_element_type=F32)
            up = jnp.dot(rows, abuf[slot1], preferred_element_type=F32)
            hbuf[0:16, :] = (silu(gate) * up).astype(BF)

        @pl.when(p == 0)
        def _():
            a_expert(7).start()
            a_expert(8).start()

        @pl.when(p == 1)
        def _():
            a_expert(9).start()

        @pl.when(p == 2)
        def _():
            b_expert(4).start()

        @pl.when(is_rest)
        def _():
            for hop in (2, 0):
                send_rows(p, hop, (s - s % 2 + hop) % 4)

        @pl.when(jnp.logical_not(is_rest))
        def _():
            pltpu.make_async_copy(wd.at[0], bbuf.at[slotb], bsem.at[slotb]).wait()

            rows = hbuf[0:16, :]
            for hop in (2, 0):
                first = (s - s % 2 + hop) % 4
                res = jnp.dot(rows, bbuf[slotb, :, pl.ds(pl.multiple_of(first * COLS, 2 * COLS), 2 * COLS)], preferred_element_type=F32)
                for side in range(2):
                    for pair in range(2):
                        left = res[span(pair, 8), COLS * side:COLS * side + 256]
                        right = res[span(pair, 8), COLS * side + 256:COLS * side + 512]
                        even = jnp.where(low, left, pltpu.roll(right, 4, axis=0))
                        odd = jnp.where(low, pltpu.roll(left, 4, axis=0), right)
                        ybuf[8 * pair + first + side, p] = even.astype(BF)
                        ybuf[8 * pair + 4 + first + side, p] = odd.astype(BF)
                send_rows(p, hop, first)

        return carry

    lax.fori_loop(0, 4, unit_body, 0)

    rbuf[4 * d + s] = ybuf[4 * d + s]
    srecv[s] = spart[s]
    arrived(spart, 3, srec)
    shared = (srecv[0] + srecv[1] + srecv[2] + srecv[3]).astype(BF).astype(F32)
    arrived(ybuf, 15, rrecv)
    got = jnp.dot(stackv[...], rbuf[...].reshape(512, 256), preferred_element_type=F32)
    got = [got[span(n, ROWS)] for n in range(6)]
    routed = jnp.concatenate([got[0] + got[1] + got[2], got[3] + got[4] + got[5]], axis=1)
    out[:, col] = (mid.astype(F32) + shared + routed).astype(BF)
    ocopies = [pltpu.make_async_remote_copy(out.at[:, col], out.at[:, col], osend, orecv,
                                            device_id={"side": (s + k) % 4}, device_id_type=MESH) for k in range(1, 4)]
    for c in ocopies:
        c.start()

    arrived(cbuf, 3, csend)
    arrived(idsx, 3, isend)
    arrived(mbuf, 15, msend)
    arrived(spart, 3, ssend)
    arrived(ybuf, 15, rsend)
    arrived(cbuf, 3, osend)
    arrived(cbuf, 3, orecv)


def solution(mesh):
    def device_fn(hidden, k_cache, v_cache, cache_lens, expert_ids, route_gates, *weights):
        any_spec = pl.BlockSpec(memory_space=pl.ANY)
        dma = pltpu.SemaphoreType.DMA
        vm = pltpu.VMEM
        return pl.pallas_call(
            kernel,
            out_shape=pltpu.VMEM((ROWS, DIM), BF),
            in_specs=[any_spec] * 17,
            out_specs=pl.BlockSpec(memory_space=pltpu.VMEM),
            scratch_shapes=[
                vm((ROWS, DIM), BF), vm((ROWS, COLS), BF), vm((1, ROWS), jnp.int32), vm((4, ROWS), jnp.int32),
                vm((4, ROWS), F32), vm((1, DIM), F32), vm((1, DIM), F32),
                vm((ROWS, HEADS, 128, 128), BF), vm((ROWS, HEADS, 128, 128), BF),
                vm((NA, DIM, FF), BF), vm((NB, FF, DIM), BF),
                vm((4, 8, 128), F32), vm((4, ROWS, COLS), BF), vm((16, ROWS, COLS), BF),
                vm((128, DIM), BF), vm((64, DIM), BF), vm((ROWS, FF), BF),
                vm((16, 4, 8, 256), BF), vm((16, 4, 8, 256), BF),
                vm((4, ROWS, COLS), F32), vm((4, ROWS, COLS), F32), vm((192, 512), BF),
                dma((7,)), dma((8,)), dma((NA,)), dma((NB,)), dma, dma, dma, dma, dma, dma((4,)), dma((4,)), dma((4,)), dma((4,)),
                dma, dma, dma, dma, dma, dma,
            ],
            compiler_params=pltpu.CompilerParams(collective_id=0, has_side_effects=True, vmem_limit_bytes=66000000),
            name="moe_decode",
        )(hidden, k_cache, v_cache, cache_lens.reshape(1, ROWS), jnp.swapaxes(expert_ids, 1, 2),
          jnp.swapaxes(route_gates, 1, 2), *weights)

    batch = P(("inst", "dev"))
    layer = P(None, ("inst", "dev"))
    expert = P(None, "dev")
    in_specs = (batch, layer, layer, batch, layer, layer) + (P(),) * 8 + (expert,) * 3
    return jax.shard_map(device_fn, mesh=mesh, in_specs=in_specs, out_specs=batch, check_vma=False)
```
